32 devices in a mesh: dp: 4 (over y, x), eng: 2 (over core), tp: 4 (over z).
Axes of the slice: x: 2, y: 2, z: 4, core: 2. Of those that a mesh axis runs over, the one named last changes fastest.
Arguments:
- grad_parts: bfloat16 [4, 4, 1024, 14336], P('dp', 'tp', None, 'eng'), may hold values from -24 to 24
- master: float32 [4, 1024, 14336], P('tp', 'dp', 'eng'), may hold values from -0.09375 to 0.09375
- first_moment: float32 [4, 1024, 14336], P('tp', 'dp', 'eng'), may hold values from -12 to 12
- second_moment: float32 [4, 1024, 14336], P('tp', 'dp', 'eng'), may hold values from 4 to 256
- adam_step: int32 [1], replicated, may hold values from 1 to 999
- rank_map: int32 [4], replicated, may hold values from 0 to 3, each once
Outputs:
- new_master: float32 [4, 1024, 14336], P('tp', 'dp', 'eng')
- new_first: float32 [4, 1024, 14336], P('tp', 'dp', 'eng')
- new_second: float32 [4, 1024, 14336], P('tp', 'dp', 'eng')
- rollout: bfloat16 [4, 1024, 2, 4, 1792], P(None, 'dp', None, 'tp')
The draws below stay inside these ranges and needn't reach their ends.
Inputs may be any that keep to these rules, and one draw needn't show every extreme that they name: `rank_map`: each of 0 to 3 appears once.
All inputs are finite; a program needn't handle non-finite values.
Results may differ from the reference program's by a relative error of at most 0.001.
Values may be sent and summed in bfloat16 or wider, within the bound.
No kernel may reach another device: no remote copies, remote signals or barrier semaphores. Data moves between devices by JAX's collectives and lax.ppermute only.
A program may use at most 192 MiB of HBM per device.

```python
import math
import jax
import jax.numpy as jnp
from jax import lax

D = 4096
F = 14336
N_DP = 4
N_ENG = 2
N_TP = 4


def with_spikes(drawn, key, source, target, parts, factor):
    def block_of(dim):
        return (jnp.arange(drawn.shape[dim]) // (drawn.shape[dim] // parts)).reshape((-1,) + (1,) * (drawn.ndim - 1 - dim))

    near = jax.random.permutation(key, parts)[block_of(target)]
    second = (block_of(target) + parts // 2) % parts
    return jnp.where((block_of(source) == near) | (block_of(source) == second), factor * drawn, drawn)


def shard_levels(rng, shape, split, low, high):
    loudness, own = 1.0, jax.random.fold_in(rng, 6)
    for dim, parts in split:
        steps = jnp.exp(jax.random.uniform(jax.random.fold_in(own, dim), (parts,), jnp.float32, low / len(split), high / len(split)))
        loudness = loudness * jnp.repeat(steps, shape[dim] // parts).reshape([-1 if axis == dim else 1 for axis in range(len(shape))])
    return loudness


def centred(rng, dims, width, limit, split=(), dtype=jnp.bfloat16):
    level = shard_levels(rng, dims, split, -0.22, 0.18) if split else 1.0
    drawn = jax.random.normal(rng, dims, jnp.float32) * width * level
    return jnp.minimum(jnp.maximum(drawn, -limit), limit).astype(dtype)


def heavy_noise(stream_key, dims, width, most, shards, heavy, kind=jnp.bfloat16):
    drawn = width * jax.random.normal(stream_key, dims, jnp.float32)
    if shards:
        drawn = drawn * shard_levels(stream_key, dims, shards, -0.22, 0.18)
    return jnp.clip(with_spikes(drawn, jax.random.fold_in(stream_key, 3), *heavy), -most, most).astype(kind)


def setup_inputs(seed: int = 0) -> dict:
    seeds = jax.random.split(jax.random.key(seed), 7)
    return {
        "grad_parts": heavy_noise(seeds[0], (N_DP, N_TP, D // N_TP, F), 4.0, 24.0, ((0, 4), (1, 4), (3, 2)), (0, 2, 4, 2.0)),
        "master": centred(seeds[1], (N_TP, D // N_TP, F), D ** -0.5, 0.09375, ((0, 4), (1, 4), (2, 2)), jnp.float32),
        "first_moment": centred(seeds[2], (N_TP, D // N_TP, F), 2.0, 12.0, ((0, 4), (1, 4), (2, 2)), jnp.float32),
        "second_moment": jnp.clip(jnp.exp(math.log(256.0) - 4.158883 * jax.random.uniform(seeds[3], (N_TP, D // N_TP, F), jnp.float32) ** shard_levels(seeds[3], (N_TP, D // N_TP, F), ((0, 4), (1, 4), (2, 2)), -0.2, 0.2)), 4.0, 256.0),
        "adam_step": jax.random.randint(seeds[4], (1,), 1, 1000).astype(jnp.int32),
        "rank_map": jax.random.permutation(seeds[5], N_TP).astype(jnp.int32),
    }


beta_one = 0.9
beta_two = 0.95
rate_value = 0.001
decay_value = 0.01
eps_value = 1e-08

def reference(grad_parts, master, first_moment, second_moment, adam_step, rank_map):
    summed = lax.optimization_barrier(jnp.sum(grad_parts.astype(jnp.float32), axis=0))
    count = adam_step[0].astype(jnp.float32)
    new_first = beta_one * first_moment + (1.0 - beta_one) * summed
    new_second = beta_two * second_moment + (1.0 - beta_two) * summed * summed
    first_hat = new_first / (1.0 - jnp.power(beta_one, count))
    second_hat = new_second / (1.0 - jnp.power(beta_two, count))
    new_master = master - rate_value * (first_hat / (jnp.sqrt(second_hat) + eps_value) + decay_value * master)
    weights = new_master.astype(jnp.bfloat16).reshape(N_TP, D // N_TP, N_ENG, N_TP, F // (N_ENG * N_TP))
    rollout = jnp.take(weights, rank_map.astype(jnp.int32), axis=3)
    return (new_master, new_first, new_second, rollout)
```

```python
import math

import jax
import jax.numpy as jnp
from jax import lax
from jax.experimental import pallas as pl
from jax.experimental.pallas import tpu as pltpu
from jax.sharding import PartitionSpec as P

beta_one = 0.9
beta_two = 0.95
rate_value = 0.001
decay_value = 0.01
eps_value = 1e-08
grad_limit = 24.0

LANES = 128
TILE = 8
SHARES = (1, 2, 3, 3, 3, 2, 2)
Z_ORDER = (2, 3, 1)
PIECES = (32, 24, 16, TILE)


def corrections_of(adam_step):
    count = adam_step[0].astype(jnp.float32)
    return 1.0 - jnp.power(jnp.array([beta_one, beta_two], jnp.float32), count)


def pair_scale():
    scale = 1.0
    while scale * 2 * 2 * grad_limit < 32767:
        scale *= 2
    return scale


def flipped(mine, side, other):
    first = 1 - ((mine >> side) & 1)
    return (first << side) + (other << (1 - side))


def piece_of(half):
    return next(p for p in PIECES if half % p == 0)


def step(rank_map, corrections, grads, states, news, rollout, send, pair, new, join, ahead_pair, ahead_new):
    columns = grads.shape[2]
    ranks = rank_map.shape[0]
    width = columns // ranks
    lanes = next(w for w in range(1024, 0, -LANES) if width % w == 0)
    scale = pair_scale()

    operands, in_specs, out_shape, out_specs, scratch, aliases = [], [], [], [], [], {}
    held = [4 << 20]
    hbm = pl.BlockSpec(memory_space=pltpu.HBM)
    vmem = pl.BlockSpec(memory_space=pltpu.VMEM)

    def give(x, spec=vmem, alias=None):
        if alias is not None:
            aliases[len(operands)] = alias
        kind = spec.memory_space
        operands.append(x if kind == pltpu.SMEM else pltpu.with_memory_space_constraint(x, kind))
        in_specs.append(spec)
        return len(operands) - 1

    def take(shape, dtype, spec=vmem):
        out_shape.append(spec.memory_space(shape, dtype))
        out_specs.append(spec)
        return len(out_shape) - 1

    def room(shape, dtype):
        scratch.append(pltpu.VMEM(shape, dtype))
        held[0] += math.prod(shape) * jnp.dtype(dtype).itemsize
        return len(scratch) - 1

    for x in (rank_map, corrections) if new else ():
        give(x, pl.BlockSpec(memory_space=pltpu.SMEM))
    grads_at = give(grads, hbm)
    if send:
        send_out = [take((2, send[1], columns), jnp.bfloat16) for _ in range(2)]
    if pair:
        pair_in = [give(x) for x in pair[2]]
        pair_out = [take((pair[1], columns), jnp.int16) for _ in range(2)]
        pair_raw = [give(x) for x in pair[3]]
    if new:
        rows = 2 * new[1]
        first_in = [give(x) for x in new[2]]
        second_in = [give(x) for x in new[3]]
        new_raw, *state_in = [give(x) for x in new[4]]
        state_out = [take(x.shape, x.dtype, hbm) for x in states]
        slot_out = [take((rows, width), jnp.bfloat16) for _ in range(ranks)]
        new_state = [room((rows, columns), jnp.float32) for _ in range(3)]
        if news:
            for at, x in zip(state_out, news):
                give(x, hbm, at)
    if ahead_pair:
        ahead_pair_out = [take((ahead_pair[1], columns), jnp.bfloat16) for _ in range(2)]
    if ahead_new:
        ahead_rows = 2 * ahead_new[1]
        ahead_in = [give(x, hbm) for x in states]
        ahead_out = [take((ahead_rows, columns), jnp.bfloat16)]
        ahead_out += [take((ahead_rows, columns), jnp.float32) for _ in states]
    if join:
        join_in = [[[give(x) for x in group] for group in part[1:]] for part in join]
        join_out = take((ranks, grads.shape[1], 2, width), jnp.bfloat16, hbm)
        join_made = [room((ranks, part[1][0].shape[0], 2, width), jnp.bfloat16) for part in join]
        if rollout is not None:
            give(rollout, hbm, join_out)

    def body(*refs):
        ins = refs[: len(operands)]
        outs = refs[len(operands) : len(operands) + len(out_shape)]
        bufs = refs[len(operands) + len(out_shape) : -1]
        sems = refs[-1]
        used = [0]
        blocks, corr = ins[:2] if new else (None, None)
        raw = ins[grads_at]
        dp, tp, eng = (lax.axis_index(axis) for axis in ("dp", "tp", "eng"))
        sending, stores = [], []

        def copy(source, target):
            made = pltpu.make_async_copy(source, target, sems.at[used[0]])
            used[0] += 1
            made.start()
            return made

        if send:
            start, half = send[:2]
            for side in range(2):
                for j in range(2):
                    rows_there = pl.ds(start + side * half, half)
                    sending.append(copy(raw.at[flipped(dp, side, j), rows_there], outs[send_out[side]].at[j]))
        if ahead_pair:
            start, half = ahead_pair
            for side in range(2):
                far = 1 - ((dp >> (1 - side)) & 1)
                owner = (((dp >> side) & 1) << side) + (far << (1 - side))
                rows_there = pl.ds(start + side * half, half)
                sending.append(copy(raw.at[owner, rows_there], outs[ahead_pair_out[side]]))
        if ahead_new:
            there = pl.ds(ahead_new[0], ahead_rows)
            sending.append(copy(raw.at[dp, there], outs[ahead_out[0]]))
            for at, target in zip(ahead_in, ahead_out[1:]):
                sending.append(copy(ins[at].at[0, there], outs[target]))
        for part, arrived, made in zip(join, join_in if join else (), join_made if join else ()):
            made_ref = bufs[made]
            for side in range(2):

                @pl.when(eng == side)
                def _():
                    for slot in range(ranks):
                        made_ref[slot, :, side, :] = ins[arrived[0][slot]][...]
                        made_ref[slot, :, 1 - side, :] = ins[arrived[1][slot]][...]

            there = pl.ds(part[0], part[1][0].shape[0])
            for slot in range(ranks):
                stores.append(copy(made_ref.at[slot], outs[join_out].at[tp ^ slot, there]))
        if pair:
            half = pair[1]
            for side in range(2):
                far = 1 - ((dp >> (1 - side)) & 1)
                mine, got, total = ins[pair_raw[side]], ins[pair_in[side]], outs[pair_out[side]]

                @pl.loop(0, half // TILE)
                def _(t):
                    at = pl.ds(pl.multiple_of(t * TILE, TILE), TILE)
                    for c in range(0, columns, lanes):
                        here = slice(c, c + lanes)
                        both = mine[at, here].astype(jnp.float32) + got[far, at, here].astype(jnp.float32)
                        total[at, here] = jnp.round(both * scale).astype(jnp.int16)

        if new:
            start, half = new[:2]
            master, first, second = (ins[at] for at in state_in)
            new_master, new_first, new_second = (bufs[b] for b in new_state)
            mine = ins[new_raw]
            by_first, by_second = corr[0], corr[1]
            piece = piece_of(half)
            for first_row in range(0, 2 * half, piece):
                side = first_row // half
                near = (dp >> (1 - side)) & 1
                one_got, two_got = ins[first_in[side]], ins[second_in[side]]

                @pl.loop(0, piece // TILE)
                def _(t):
                    at = pl.ds(pl.multiple_of(first_row + t * TILE, TILE), TILE)
                    inner = pl.ds(pl.multiple_of(first_row - side * half + t * TILE, TILE), TILE)
                    for slot in range(ranks):
                        block = blocks[tp ^ slot] * width
                        for c in range(0, width, lanes):
                            here = pl.ds(pl.multiple_of(block + c, LANES), lanes)
                            summed = (
                                mine[at, here].astype(jnp.float32)
                                + one_got[near, inner, here].astype(jnp.float32)
                                + two_got[inner, here].astype(jnp.float32) * (1.0 / scale)
                            )
                            one = beta_one * first[at, here] + (1.0 - beta_one) * summed
                            two = beta_two * second[at, here] + (1.0 - beta_two) * summed * summed
                            old = master[at, here]
                            now = old - rate_value * (
                                (one * by_first) / (jnp.sqrt(two * by_second) + eps_value) + decay_value * old
                            )
                            new_first[at, here] = one
                            new_second[at, here] = two
                            new_master[at, here] = now
                            outs[slot_out[slot]][at, c : c + lanes] = now.astype(jnp.bfloat16)

                part = pl.ds(first_row, piece)
                for b, at in zip(new_state, state_out):
                    stores.append(copy(bufs[b].at[part], outs[at].at[0, pl.ds(start + first_row, piece)]))
        for made in sending + stores:
            made.wait()

    pieces = 2 * new[1] // piece_of(new[1]) if new else 0
    copies = (4 if send else 0) + (2 if ahead_pair else 0) + (4 if ahead_new else 0) + 3 * pieces
    copies += ranks * len(join)
    got = pl.pallas_call(
        body,
        in_specs=in_specs,
        out_specs=out_specs,
        out_shape=out_shape,
        scratch_shapes=scratch + [pltpu.SemaphoreType.DMA((copies,))],
        input_output_aliases=aliases,
        compiler_params=pltpu.CompilerParams(vmem_limit_bytes=held[0]),
    )(*operands)
    result = {}
    if send:
        result["send"] = [got[at] for at in send_out]
    if pair:
        result["pair"] = [got[at] for at in pair_out]
    if new:
        result["new"] = ([got[at] for at in state_out], [got[at] for at in slot_out])
    if join:
        result["join"] = got[join_out]
    if ahead_pair:
        result["ahead_pair"] = [got[at] for at in ahead_pair_out]
    if ahead_new:
        result["ahead_new"] = [got[at] for at in ahead_out]
    return result


def pipelined(grad_parts, master, first_moment, second_moment, adam_step, rank_map):
    _, row_count, columns = master.shape
    ranks = lax.axis_size("tp")
    width = columns // ranks
    grads = grad_parts.reshape(4, row_count, columns)
    states = (master, first_moment, second_moment)
    by = None
    unit = row_count // sum(SHARES)
    sizes = [unit * s for s in SHARES]
    starts = [sum(sizes[:i]) for i in range(len(sizes))]
    chunks = len(sizes)
    news, rollout = None, None
    round_one, round_two = {}, {}
    ours, theirs = {}, {}
    blocks = rank_map.astype(jnp.int32)

    def swap(x, axis, flip):
        return lax.ppermute(x, axis, [(d, d ^ flip) for d in range(lax.axis_size(axis))])

    def stage(send, pair, new, join, ahead_pair, ahead_new):
        nonlocal news, rollout, by
        done = step(
            blocks,
            jnp.ones((2,), jnp.float32) if by is None else by,
            grads,
            states,
            news,
            rollout,
            None if send is None else (starts[send], sizes[send] // 2),
            None if pair is None else (starts[pair], sizes[pair] // 2, round_one[pair], fetched_pair[pair]),
            None if new is None else (starts[new], sizes[new] // 2, round_one[new], round_two[new], fetched[new]),
            [(starts[j], ours[j], theirs[j]) for j in join],
            None if ahead_pair is None else (starts[ahead_pair], sizes[ahead_pair] // 2),
            None if ahead_new is None else (starts[ahead_new], sizes[ahead_new] // 2),
        )
        if by is None:
            late, _ = lax.optimization_barrier((adam_step, done["send"][0]))
            by = 1.0 / corrections_of(late)
        if send is not None:
            held[send] = done["send"]
        if pair is not None:
            sums[pair] = done["pair"]
        if new is not None:
            news, slots[new] = done["new"]
        if join:
            rollout = done["join"]
        if ahead_pair is not None:
            fetched_pair[ahead_pair] = done["ahead_pair"]
        if ahead_new is not None:
            fetched[ahead_new] = done["ahead_new"]

    held, sums, slots, fetched, fetched_pair = {}, {}, {}, {}, {}
    for kind, *what in plan(chunks):
        if kind == "stage":
            stage(*what)
            continue
        i, s = what
        if kind == "p1":
            round_one.setdefault(i, [None] * 2)[s] = swap(held[i][s], "dp", 1 << s)
        elif kind == "p2":
            round_two.setdefault(i, [None] * 2)[s] = swap(sums[i][s], "dp", 2 >> s)
        elif kind == "z":
            ours.setdefault(i, [slots[i][0]] + [None] * (ranks - 1))[s] = swap(slots[i][s], "tp", s)
        else:
            mine = ours[i][s] if i in ours else slots[i][s]
            theirs.setdefault(i, [None] * ranks)[s] = swap(mine, "eng", 1)
    return (*news, rollout.reshape(ranks, row_count, 2, 1, width))


def general(grad_parts, master, first_moment, second_moment, adam_step, rank_map):
    replicas, ranks = lax.axis_size("dp"), lax.axis_size("tp")
    _, row_count, columns = master.shape
    parts = grad_parts.reshape(replicas, row_count, columns).astype(jnp.float32)
    summed = lax.psum_scatter(parts, "dp", scatter_dimension=0, tiled=True)
    by = corrections_of(adam_step)
    new_first = beta_one * first_moment + (1.0 - beta_one) * summed
    new_second = beta_two * second_moment + (1.0 - beta_two) * summed * summed
    new_master = master - rate_value * (
        (new_first / by[0]) / (jnp.sqrt(new_second / by[1]) + eps_value) + decay_value * master
    )
    piece = new_master.astype(jnp.bfloat16).reshape(1, row_count, 1, ranks, columns // ranks)
    ordered = jnp.take(piece, rank_map, axis=3)
    placed = lax.all_to_all(ordered, "tp", split_axis=3, concat_axis=0, tiled=True)
    rollout = lax.all_gather(placed, "eng", axis=2, tiled=True)
    return (new_master, new_first, new_second, rollout)


def plan(chunks):
    events = []

    def known(i):
        return i if 0 <= i < chunks else None

    def stage(send=None, pair=None, new=None, join=()):
        parts = (known(-1 if send is None else send), pair, new, tuple(j for j in join if known(j) is not None))
        if parts != (None, None, None, ()):
            events.append(("stage", *parts))

    def start(kind, i, which):
        if known(i) is not None:
            events.extend((kind, i, s) for s in which)

    across = Z_ORDER
    stage(send=0)
    start("p1", 0, (0, 1))
    stage(send=1)
    start("p1", 1, (0, 1))
    last = chunks - 1
    for i in range(last):
        stage(i + 2, i, known(i - 1), (i - 3,) if i < last - 1 else ())
        start("p2", i, (1, 0))
        start("z", i - 1, across)
        start("p1", i + 2, (0, 1))
        if i < last - 1:
            start("e", i - 1, (0,))
            start("e", i - 2, across)
    stage(pair=last)
    start("p2", last, (1, 0))
    stage(new=last - 1)
    start("z", last - 1, across)
    stage(new=last)
    start("z", last, across)
    start("e", last - 3, across)
    for i in (last - 2, last - 1):
        start("e", i, (0,))
    start("e", last - 2, across)
    start("e", last, (0,))
    stage(join=(last - 4, last - 3, last - 2))
    start("e", last - 1, across)
    stage(join=(last - 1,))
    start("e", last, across)
    stage(join=(last,))
    ahead = (None, None)
    for at in reversed(range(len(events))):
        if events[at][0] == "stage":
            pair, new = events[at][2:4]
            events[at] += ahead
            ahead = (pair, new)
    return events


def solution(mesh):
    shape = dict(mesh.shape)
    direct = (shape["dp"], shape["eng"]) == (4, 2) and shape["tp"] == 4

    def shards(*args):
        if not direct:
            return general(*args)
        return pipelined(*args)

    return jax.shard_map(
        shards,
        mesh=mesh,
        in_specs=(
            P("dp", "tp", None, "eng"),
            P("tp", "dp", "eng"),
            P("tp", "dp", "eng"),
            P("tp", "dp", "eng"),
            P(),
            P(),
        ),
        out_specs=(
            P("tp", "dp", "eng"),
            P("tp", "dp", "eng"),
            P("tp", "dp", "eng"),
            P(None, "dp", None, "tp", None),
        ),
        check_vma=False,
    )
```
